32 devices in a mesh: ty: 8 (over z, y), tx: 4 (over x, core).
Axes of the slice: x: 2, y: 2, z: 4, core: 2. Of those that a mesh axis runs over, the one named last changes fastest.
Arguments:
- w_in: float32 [4, 8, 2, 256, 1024], P('tx', 'ty')
- w_out: float32 [4, 8, 2, 1024, 256], P('tx', 'ty')
- inputs: bfloat16 [4, 8, 9, 2048, 256], P('tx', 'ty')
- targets: bfloat16 [4, 8, 9, 2048, 256], P('tx', 'ty')
Outputs:
- output 1: float32 [4, 8, 2, 256, 1024], P('tx', 'ty')
- output 2: float32 [4, 8, 2, 1024, 256], P('tx', 'ty')
- output 3: float32 [4, 8, 2, 256, 1024], P('tx', 'ty')
- output 4: float32 [4, 8, 2, 1024, 256], P('tx', 'ty')
All inputs are finite; a program needn't handle non-finite values.
Results may differ from the reference program's by a relative error of at most 0.00727995.
Values are sent between devices in bfloat16 or wider.
A program may use at most 1 GiB of HBM per device.

```python
import jax
import jax.numpy as jnp
from jax import lax

TX = 4
TY = 8
LAYERS = 2
D = 256
FF = 1024
ROWS = 2048
STEPS = 8
EPS = 1e-6
LEARN_RATE = 0.125


def setup_inputs(seed: int = 0) -> dict:
    root_key = jax.random.key(seed)
    key_list = jax.random.split(root_key, 6)
    base_in = jax.random.normal(key_list[0], (LAYERS, D, FF), jnp.float32)
    own_in = jax.random.normal(key_list[1], (TX, TY, LAYERS, D, FF), jnp.float32)
    w_in = (base_in[None, None] + 0.5 * own_in) * (D ** -0.5)
    base_out = jax.random.normal(key_list[2], (LAYERS, FF, D), jnp.float32)
    own_out = jax.random.normal(key_list[3], (TX, TY, LAYERS, FF, D), jnp.float32)
    w_out = (base_out[None, None] + 0.5 * own_out) * (FF ** -0.5)
    inputs = jax.random.normal(key_list[4], (TX, TY, STEPS + 1, ROWS, D), jnp.float32).astype(jnp.bfloat16)
    targets = jax.random.normal(key_list[5], (TX, TY, STEPS + 1, ROWS, D), jnp.float32).astype(jnp.bfloat16)
    return {'w_in': w_in, 'w_out': w_out, 'inputs': inputs, 'targets': targets}


def layer_step(hidden, weights):
    mat_in, mat_out = weights
    hidden_f32 = hidden.astype(jnp.float32)
    inv_rms = lax.rsqrt(jnp.mean(hidden_f32 * hidden_f32, axis=-1, keepdims=True) + EPS)
    normed = (hidden_f32 * inv_rms).astype(jnp.bfloat16)
    pre_act = jnp.dot(normed, mat_in.astype(jnp.bfloat16), preferred_element_type=jnp.float32)
    gelu_out = jax.nn.gelu(pre_act).astype(jnp.bfloat16)
    mlp_out = jnp.dot(gelu_out, mat_out.astype(jnp.bfloat16), preferred_element_type=jnp.float32)
    return (hidden_f32 + mlp_out).astype(jnp.bfloat16), None


def local_loss(w_in, w_out, batch_in, batch_tgt):
    last_hidden, _ = lax.scan(layer_step, batch_in, (w_in, w_out))
    resid_err = last_hidden.astype(jnp.float32) - batch_tgt.astype(jnp.float32)
    return jnp.mean(resid_err * resid_err)


local_grads = jax.grad(local_loss, argnums=(0, 1))


def gossip_mix(values):
    sent_copy = values.astype(jnp.bfloat16).astype(jnp.float32)
    summed = values + jnp.roll(sent_copy, 1, axis=0)
    summed = summed + jnp.roll(sent_copy, -1, axis=0)
    summed = summed + jnp.roll(sent_copy, 1, axis=1)
    summed = summed + jnp.roll(sent_copy, -1, axis=1)
    return summed / 5.0


def reference(w_in, w_out, inputs, targets):
    cell_count = TX * TY
    step_size = LEARN_RATE

    def one_cell(operands):
        return local_grads(operands[0], operands[1], operands[2], operands[3])

    def all_grads(p_in, p_out, step_idx):
        batch_in = lax.dynamic_index_in_dim(inputs, step_idx, axis=2, keepdims=False).reshape((cell_count, ROWS, D))
        batch_tgt = lax.dynamic_index_in_dim(targets, step_idx, axis=2, keepdims=False).reshape((cell_count, ROWS, D))
        grad_in, grad_out = lax.map(one_cell, (p_in.reshape((cell_count, LAYERS, D, FF)), p_out.reshape((cell_count, LAYERS, FF, D)), batch_in, batch_tgt))
        return grad_in.reshape(p_in.shape), grad_out.reshape(p_out.shape)

    first_in, first_out = all_grads(w_in, w_out, 0)

    def step_body(carried, step_idx):
        p_in, p_out, y_in, y_out, old_in, old_out = carried
        p_in = gossip_mix(p_in) - step_size * y_in
        p_out = gossip_mix(p_out) - step_size * y_out
        new_gin, new_gout = all_grads(p_in, p_out, step_idx)
        y_in = gossip_mix(y_in) + new_gin - old_in
        y_out = gossip_mix(y_out) + new_gout - old_out
        return (p_in, p_out, y_in, y_out, new_gin, new_gout), None

    final_state, _ = lax.scan(step_body, (w_in, w_out, first_in, first_out, first_in, first_out), jnp.arange(1, STEPS + 1))
    return (final_state[0], final_state[1], final_state[2], final_state[3])
```

```python
import functools

import jax
import jax.numpy as jnp
from jax import lax
from jax.experimental import pallas as pl
from jax.experimental.pallas import tpu as pltpu
from jax.sharding import PartitionSpec as P

EPS = 1e-6
LEARN_RATE = 0.125
UNITS = 8
BLOCKS = 8
GELU_C0 = 0.7978845608028654
GELU_C1 = 0.044715 * GELU_C0
F32 = jnp.float32
BF16 = jnp.bfloat16
MESH = pl.DeviceIdType.MESH


def dot(lhs, rhs, lhs_dim, rhs_dim):
    return lax.dot_general(lhs, rhs, (((lhs_dim,), (rhs_dim,)), ((), ())), preferred_element_type=F32)


def kernel(dims, win_hbm, wout_hbm, x_hbm, tgt_hbm, pin_hbm, pout_hbm, yin_hbm, yout_hbm,
           p_in, p_out, y_in, y_out, acc_in, acc_out, old_in, old_out,
           send_in, send_out, recv_in, recv_out, x_v, tgt_v, gp, act, unit_in, tmp, dz,
           recv_sem, send_sem, load_sem, store_sem):
    n_x, n_y, layers, d, ff, steps, rows = dims
    rb_rows = rows // BLOCKS
    ix, iy = lax.axis_index('tx'), lax.axis_index('ty')
    px, py = ix % 2, iy % 2
    partner = ix + 1 - 2 * px
    opposite = n_x - 1 - ix
    y_partner = iy + 1 - 2 * py
    relay_to = (iy + 2 * (1 - 2 * py) + n_y) % n_y
    relay_from = (iy - 2 * (1 - 2 * py) + n_y) % n_y
    to_partner = {'tx': partner, 'ty': iy}
    to_opposite = {'tx': opposite, 'ty': iy}
    to_y = {'tx': ix, 'ty': y_partner}
    to_z = {'tx': ix, 'ty': relay_to}
    y_dir = 3 - py
    z_dir = 2 + py

    barrier = pltpu.get_barrier_semaphore()
    for peer in (to_partner, to_opposite, to_y, to_z, {'tx': ix, 'ty': relay_from}):
        pl.semaphore_signal(barrier, inc=1, device_id=peer, device_id_type=MESH)

    piece = ((layers * d) // UNITS, (layers * ff) // UNITS)
    sends = (send_in, send_out)
    recvs = (recv_in, recv_out)

    def span(side, unit):
        return pl.ds(pl.multiple_of(unit * piece[side], piece[side]), piece[side])

    def direct(side, kind, unit, slot, dest):
        peer, where = ((to_partner, px), (to_opposite, 1 - px), (to_y, 2 + py))[dest]
        at = span(side, unit)
        return pltpu.make_async_remote_copy(
            src_ref=sends[side].at[kind, at],
            dst_ref=recvs[side].at[slot, kind, where, at],
            send_sem=send_sem.at[side, kind, unit, dest],
            recv_sem=recv_sem.at[side, slot, kind, unit, where],
            device_id=peer, device_id_type=MESH)

    def relay(side, kind, unit, slot):
        at = span(side, unit)
        return pltpu.make_async_remote_copy(
            src_ref=recvs[side].at[slot, kind, y_dir, at],
            dst_ref=recvs[side].at[slot, kind, z_dir, at],
            send_sem=send_sem.at[side, kind, unit, 3],
            recv_sem=recv_sem.at[side, slot, kind, unit, z_dir],
            device_id=to_z, device_id_type=MESH)

    def arrival(side, kind, unit, slot, where):
        at = span(side, unit)
        return pltpu.make_async_remote_copy(
            src_ref=sends[side].at[kind, at],
            dst_ref=recvs[side].at[slot, kind, where, at],
            send_sem=send_sem.at[side, kind, unit, 0],
            recv_sem=recv_sem.at[side, slot, kind, unit, where],
            device_id=to_partner, device_id_type=MESH)

    def send_piece(kind, unit, slot):
        for side in (0, 1):
            for dest in (2, 1, 0):
                direct(side, kind, unit, slot, dest).start()

    def forward(side, kind, unit, slot):
        arrival(side, kind, unit, slot, y_dir).wait_recv()
        relay(side, kind, unit, slot).start()

    def settle(kind, unit, slot):
        for side in (0, 1):
            for where in (0, 1, z_dir):
                arrival(side, kind, unit, slot, where).wait_recv()
            for dest in (0, 1, 2):
                direct(side, kind, unit, slot, dest).wait_send()
            relay(side, kind, unit, slot).wait_send()

    def batch_copies(step):
        return (pltpu.make_async_copy(x_hbm.at[step], x_v, load_sem.at[0]),
                pltpu.make_async_copy(tgt_hbm.at[step], tgt_v, load_sem.at[1]))

    weight_copies = (pltpu.make_async_copy(win_hbm, p_in, load_sem.at[2]),
                     pltpu.make_async_copy(wout_hbm, p_out, load_sem.at[3]))
    for copy in weight_copies + batch_copies(0):
        copy.start()
    for copy in weight_copies:
        copy.wait()

    def first_cast(unit, _):
        for side, weights in ((0, p_in), (1, p_out)):
            at = span(side, unit)
            sends[side][0, at] = weights[at].astype(BF16)
        return 0

    lax.fori_loop(0, UNITS, first_cast, 0)
    pl.semaphore_wait(barrier, 5)

    def first_send(unit, _):
        send_piece(0, unit, 0)
        return 0

    lax.fori_loop(0, UNITS, first_send, 0)

    def forward_layer(layer, hidden):
        w_in = send_in[0, layer * d:(layer + 1) * d]
        w_out = send_out[0, layer * ff:(layer + 1) * ff]
        inv_rms = lax.rsqrt(jnp.mean(hidden * hidden, axis=-1, keepdims=True) + EPS)
        normed = (hidden * inv_rms).astype(BF16)
        unit_in[layer] = normed
        gp[layer] = dot(normed, w_in, 1, 0)

        def activate(i, _):
            at = pl.ds(pl.multiple_of(i * 16, 16), 16)
            z = gp[layer, at]
            z2 = z * z
            tanh = jnp.tanh(z * (GELU_C0 + GELU_C1 * z2))
            cdf = 0.5 + 0.5 * tanh
            act[layer, at] = (z * cdf).astype(BF16)
            gp[layer, at] = cdf + (0.5 * z * (1.0 - tanh * tanh)) * (GELU_C0 + (3.0 * GELU_C1) * z2)
            return 0

        lax.fori_loop(0, rb_rows // 16, activate, 0)
        out = dot(act[layer], w_out, 1, 0)
        return (hidden + out).astype(BF16).astype(F32), inv_rms

    def backward_layer(layer, grad_b, hidden, inv_rms):
        w_in = send_in[0, layer * d:(layer + 1) * d]
        w_out = send_out[0, layer * ff:(layer + 1) * ff]
        tmp[...] = dot(grad_b, w_out, 1, 1)

        def chain(i, _):
            at = pl.ds(pl.multiple_of(i * 16, 16), 16)
            dz[at] = (tmp[at].astype(BF16).astype(F32) * gp[layer, at]).astype(BF16)
            return 0

        lax.fori_loop(0, rb_rows // 16, chain, 0)
        acc_out[layer * ff:(layer + 1) * ff] += dot(act[layer], grad_b, 0, 0)
        acc_in[layer * d:(layer + 1) * d] += dot(unit_in[layer], dz[...], 0, 0)
        if layer == 0:
            return None
        du = dot(dz[...], w_in, 1, 1).astype(BF16).astype(F32)
        proj = jnp.sum(du * hidden, axis=-1, keepdims=True) * (1.0 / d)
        grad = grad_b.astype(F32) + (du * inv_rms - hidden * (proj * (inv_rms * inv_rms * inv_rms)))
        return grad.astype(BF16)

    def phase(step, _):
        slot = step % 2
        for copy in batch_copies(step):
            copy.wait()
        acc_in[...] = jnp.zeros_like(acc_in)
        acc_out[...] = jnp.zeros_like(acc_out)
        edge = jnp.logical_or(step == 0, step == steps)

        def block(rb, _):
            kind = jnp.where(step == 0, 0, jnp.where(step == steps, 1, rb % 2))
            unit = jnp.where(edge, rb, rb // 2)
            at = pl.ds(pl.multiple_of(rb * rb_rows, rb_rows), rb_rows)
            hidden = [x_v[at].astype(F32)]
            scales = []
            for layer in range(layers):
                nxt, inv_rms = forward_layer(layer, hidden[-1])
                hidden.append(nxt)
                scales.append(inv_rms)
            forward(0, kind, unit, slot)
            grad = ((hidden[-1] - tgt_v[at].astype(F32)) * (2.0 / (rows * d))).astype(BF16)
            for layer in reversed(range(layers)):
                grad = backward_layer(layer, grad, hidden[layer], scales[layer])
            forward(1, kind, unit, slot)
            return 0

        lax.fori_loop(0, BLOCKS, block, 0)

        @pl.when(step < steps)
        def _():
            for copy in batch_copies(step + 1):
                copy.start()

        def update(unit, first, last):
            for side, sub, p, y, acc, old in ((0, 16, p_in, y_in, acc_in, old_in),
                                              (1, 64, p_out, y_out, acc_out, old_out)):
                def piece_step(s, _, side=side, sub=sub, p=p, y=y, acc=acc, old=old):
                    at = pl.ds(pl.multiple_of(unit * piece[side] + s * sub, sub), sub)

                    def mix(total, kind):
                        for where in range(4):
                            total = total + recvs[side][slot, kind, where, at].astype(F32)
                        return total / 5.0

                    g_b = acc[at].astype(BF16)
                    g = g_b.astype(F32)
                    if first:
                        tracker = g
                    else:
                        tracker = (mix(y[at], 1) + g) - old[at].astype(F32)
                    y[at] = tracker
                    if not last:
                        old[at] = g_b
                        weights = mix(p[at], 0) - LEARN_RATE * tracker
                        p[at] = weights
                        sends[side][0, at] = weights.astype(BF16)
                        sends[side][1, at] = tracker.astype(BF16)
                    return 0

                lax.fori_loop(0, piece[side] // sub, piece_step, 0)

        def unit_step(unit, _):
            @pl.when(step < steps)
            def _():
                settle(0, unit, slot)

            @pl.when(step > 0)
            def _():
                settle(1, unit, slot)

            @pl.when(step == 0)
            def _():
                update(unit, True, False)

            @pl.when(jnp.logical_not(edge))
            def _():
                update(unit, False, False)

            @pl.when(step == steps)
            def _():
                update(unit, False, True)

            @pl.when(step < steps - 1)
            def _():
                send_piece(0, unit, 1 - slot)

            @pl.when(step < steps)
            def _():
                send_piece(1, unit, 1 - slot)

            @pl.when(jnp.logical_and(jnp.logical_not(edge), unit < UNITS // 2))
            def _():
                for kind in (0, 1):
                    for side in (0, 1):
                        forward(side, kind, unit + UNITS // 2, slot)

            return 0

        lax.fori_loop(0, UNITS, unit_step, 0)
        return 0

    lax.fori_loop(0, steps + 1, phase, 0)
    stores = [pltpu.make_async_copy(src, dst, store_sem.at[k]) for k, (src, dst) in enumerate(
        ((p_in, pin_hbm), (p_out, pout_hbm), (y_in, yin_hbm), (y_out, yout_hbm)))]
    for copy in stores:
        copy.start()
    for copy in stores:
        copy.wait()


def solution(mesh):
    n_x, n_y = mesh.shape['tx'], mesh.shape['ty']

    def device_fn(w_in, w_out, inputs, targets):
        layers, d, ff = w_in.shape[2:]
        batches, rows = inputs.shape[2:4]
        dims = (n_x, n_y, layers, d, ff, batches - 1, rows)
        s_in, s_out = (layers * d, ff), (layers * ff, d)
        rb_rows = rows // BLOCKS
        vmem = pltpu.VMEM
        outs = pl.pallas_call(
            functools.partial(kernel, dims),
            out_shape=[jax.ShapeDtypeStruct(s, F32) for s in (s_in, s_out, s_in, s_out)],
            in_specs=[pl.BlockSpec(memory_space=pl.ANY)] * 4,
            out_specs=[pl.BlockSpec(memory_space=pl.ANY)] * 4,
            scratch_shapes=[
                vmem(s_in, F32), vmem(s_out, F32), vmem(s_in, F32), vmem(s_out, F32),
                vmem(s_in, F32), vmem(s_out, F32), vmem(s_in, BF16), vmem(s_out, BF16),
                vmem((2,) + s_in, BF16), vmem((2,) + s_out, BF16),
                vmem((2, 2, 4) + s_in, BF16), vmem((2, 2, 4) + s_out, BF16),
                vmem((rows, d), BF16), vmem((rows, d), BF16),
                vmem((layers, rb_rows, ff), F32), vmem((layers, rb_rows, ff), BF16),
                vmem((layers, rb_rows, d), BF16), vmem((rb_rows, ff), F32), vmem((rb_rows, ff), BF16),
                pltpu.SemaphoreType.DMA((2, 2, 2, UNITS, 4)),
                pltpu.SemaphoreType.DMA((2, 2, UNITS, 4)),
                pltpu.SemaphoreType.DMA((4,)),
                pltpu.SemaphoreType.DMA((4,)),
            ],
            compiler_params=pltpu.CompilerParams(
                collective_id=0, has_side_effects=True, vmem_limit_bytes=67043328),
        )(w_in.reshape(s_in), w_out.reshape(s_out), inputs[0, 0], targets[0, 0])
        return tuple(o.reshape(w.shape) for o, w in zip(outs, (w_in, w_out, w_in, w_out)))

    block_spec = P('tx', 'ty')
    return jax.shard_map(device_fn, mesh=mesh, in_specs=(block_spec,) * 4, out_specs=(block_spec,) * 4, check_vma=False)
```

```python
import functools

import jax
import jax.numpy as jnp
from jax import lax
from jax.experimental import pallas as pl
from jax.experimental.pallas import tpu as pltpu
from jax.sharding import PartitionSpec as P

EPS = 1e-6
LEARN_RATE = 0.125
VMEM_LIMIT = 54 * 1024 * 1024
UNITS = 8
BLOCKS = 8
GELU_C0 = 0.7978845608028654
GELU_C1 = 0.044715 * GELU_C0
F32 = jnp.float32
BF16 = jnp.bfloat16
MESH = pl.DeviceIdType.MESH


def dot(lhs, rhs, lhs_dim, rhs_dim):
    return lax.dot_general(lhs, rhs, (((lhs_dim,), (rhs_dim,)), ((), ())), preferred_element_type=F32)


def kernel(dims, win_hbm, wout_hbm, x_hbm, tgt_hbm, p_in, p_out, y_in, y_out, acc_in, acc_out, old_in, old_out,
           send_in, send_out, recv_in, recv_out, x_v, tgt_v, gp, act, unit_in, tmp, dz,
           recv_sem, send_sem, load_sem, weight_sem):
    n_x, n_y, layers, d, ff, steps, rows = dims
    rb_rows = rows // BLOCKS
    ix, iy = lax.axis_index('tx'), lax.axis_index('ty')
    px, py = ix % 2, iy % 2
    partner = ix + 1 - 2 * px
    opposite = n_x - 1 - ix
    y_partner = iy + 1 - 2 * py
    relay_to = (iy + 2 * (1 - 2 * py) + n_y) % n_y
    relay_from = (iy - 2 * (1 - 2 * py) + n_y) % n_y
    to_partner = {'tx': partner, 'ty': iy}
    to_opposite = {'tx': opposite, 'ty': iy}
    to_y = {'tx': ix, 'ty': y_partner}
    to_z = {'tx': ix, 'ty': relay_to}
    y_dir = 3 - py
    z_dir = 2 + py

    barrier = pltpu.get_barrier_semaphore()
    for peer in (to_partner, to_opposite, to_y, to_z, {'tx': ix, 'ty': relay_from}):
        pl.semaphore_signal(barrier, inc=1, device_id=peer, device_id_type=MESH)

    piece = ((layers * d) // UNITS, (layers * ff) // UNITS)
    sends = (send_in, send_out)
    recvs = (recv_in, recv_out)

    def span(side, unit):
        return pl.ds(pl.multiple_of(unit * piece[side], piece[side]), piece[side])

    def direct(side, kind, unit, slot, dest):
        peer, where = ((to_partner, px), (to_opposite, 1 - px), (to_y, 2 + py))[dest]
        at = span(side, unit)
        return pltpu.make_async_remote_copy(
            src_ref=sends[side].at[kind, at],
            dst_ref=recvs[side].at[slot, kind, where, at],
            send_sem=send_sem.at[side, kind, unit, dest],
            recv_sem=recv_sem.at[side, slot, kind, unit, where],
            device_id=peer, device_id_type=MESH)

    def relay(side, kind, unit, slot):
        at = span(side, unit)
        return pltpu.make_async_remote_copy(
            src_ref=recvs[side].at[slot, kind, y_dir, at],
            dst_ref=recvs[side].at[slot, kind, z_dir, at],
            send_sem=send_sem.at[side, kind, unit, 3],
            recv_sem=recv_sem.at[side, slot, kind, unit, z_dir],
            device_id=to_z, device_id_type=MESH)

    def arrival(side, kind, unit, slot, where):
        at = span(side, unit)
        return pltpu.make_async_remote_copy(
            src_ref=sends[side].at[kind, at],
            dst_ref=recvs[side].at[slot, kind, where, at],
            send_sem=send_sem.at[side, kind, unit, 0],
            recv_sem=recv_sem.at[side, slot, kind, unit, where],
            device_id=to_partner, device_id_type=MESH)

    def send_piece(kind, unit, slot):
        for side in (0, 1):
            for dest in (2, 1, 0):
                direct(side, kind, unit, slot, dest).start()

    def forward(side, kind, unit, slot):
        arrival(side, kind, unit, slot, y_dir).wait_recv()
        relay(side, kind, unit, slot).start()

    def settle(kind, unit, slot):
        for side in (0, 1):
            for where in (0, 1, z_dir):
                arrival(side, kind, unit, slot, where).wait_recv()
            for dest in (0, 1, 2):
                direct(side, kind, unit, slot, dest).wait_send()
            relay(side, kind, unit, slot).wait_send()

    def batch_copies(step):
        return (pltpu.make_async_copy(x_hbm.at[step], x_v, load_sem.at[0]),
                pltpu.make_async_copy(tgt_hbm.at[step], tgt_v, load_sem.at[1]))

    def weight_copies(unit):
        return [pltpu.make_async_copy(src.at[span(side, unit)], dst.at[span(side, unit)], weight_sem.at[side, unit])
                for side, src, dst in ((0, win_hbm, p_in), (1, wout_hbm, p_out))]

    def first_load(unit, _):
        for copy in weight_copies(unit):
            copy.start()
        return 0

    lax.fori_loop(0, UNITS, first_load, 0)
    for copy in batch_copies(0):
        copy.start()

    def first_cast(unit):
        for copy in weight_copies(unit):
            copy.wait()
        for side, weights in ((0, p_in), (1, p_out)):
            at = span(side, unit)
            sends[side][0, at] = weights[at].astype(BF16)

    first_cast(0)
    pl.semaphore_wait(barrier, 5)

    def first_send(unit, _):
        @pl.when(unit > 0)
        def _():
            first_cast(unit)

        send_piece(0, unit, 0)
        return 0

    lax.fori_loop(0, UNITS, first_send, 0)

    def forward_layer(layer, hidden):
        w_in = send_in[0, layer * d:(layer + 1) * d]
        w_out = send_out[0, layer * ff:(layer + 1) * ff]
        inv_rms = lax.rsqrt(jnp.mean(hidden * hidden, axis=-1, keepdims=True) + EPS)
        normed = (hidden * inv_rms).astype(BF16)
        unit_in[layer] = normed
        gp[layer] = dot(normed, w_in, 1, 0)

        def activate(i, _):
            at = pl.ds(pl.multiple_of(i * 16, 16), 16)
            z = gp[layer, at]
            z2 = z * z
            tanh = jnp.tanh(z * (GELU_C0 + GELU_C1 * z2))
            cdf = 0.5 + 0.5 * tanh
            act[layer, at] = (z * cdf).astype(BF16)
            gp[layer, at] = cdf + (0.5 * z * (1.0 - tanh * tanh)) * (GELU_C0 + (3.0 * GELU_C1) * z2)
            return 0

        lax.fori_loop(0, rb_rows // 16, activate, 0)
        out = dot(act[layer], w_out, 1, 0)
        return (hidden + out).astype(BF16).astype(F32), inv_rms

    def backward_layer(layer, grad_b, hidden, inv_rms):
        w_in = send_in[0, layer * d:(layer + 1) * d]
        w_out = send_out[0, layer * ff:(layer + 1) * ff]
        tmp[...] = dot(grad_b, w_out, 1, 1)

        def chain(i, _):
            at = pl.ds(pl.multiple_of(i * 16, 16), 16)
            dz[at] = (tmp[at].astype(BF16).astype(F32) * gp[layer, at]).astype(BF16)
            return 0

        lax.fori_loop(0, rb_rows // 16, chain, 0)
        acc_out[layer * ff:(layer + 1) * ff] += dot(act[layer], grad_b, 0, 0)
        acc_in[layer * d:(layer + 1) * d] += dot(unit_in[layer], dz[...], 0, 0)
        if layer == 0:
            return None
        du = dot(dz[...], w_in, 1, 1).astype(BF16).astype(F32)
        proj = jnp.sum(du * hidden, axis=-1, keepdims=True) * (1.0 / d)
        grad = grad_b.astype(F32) + (du * inv_rms - hidden * (proj * (inv_rms * inv_rms * inv_rms)))
        return grad.astype(BF16)

    def phase(step, _):
        slot = step % 2
        for copy in batch_copies(step):
            copy.wait()
        acc_in[...] = jnp.zeros_like(acc_in)
        acc_out[...] = jnp.zeros_like(acc_out)
        edge = jnp.logical_or(step == 0, step == steps)

        def block(rb, _):
            pair = jnp.where(step == 0, rb, rb + 1)
            kind = jnp.where(step == 0, 0, jnp.where(step == steps, 1, pair % 2))
            unit = jnp.where(edge, pair, pair // 2)
            more = jnp.logical_or(step < steps, rb < BLOCKS - 1)
            at = pl.ds(pl.multiple_of(rb * rb_rows, rb_rows), rb_rows)
            hidden = [x_v[at].astype(F32)]
            scales = []
            for layer in range(layers):
                nxt, inv_rms = forward_layer(layer, hidden[-1])
                hidden.append(nxt)
                scales.append(inv_rms)

            @pl.when(more)
            def _():
                forward(0, kind, unit, slot)

            grad = ((hidden[-1] - tgt_v[at].astype(F32)) * (2.0 / (rows * d))).astype(BF16)
            for layer in reversed(range(layers)):
                grad = backward_layer(layer, grad, hidden[layer], scales[layer])

            @pl.when(more)
            def _():
                forward(1, kind, unit, slot)

            return 0

        lax.fori_loop(0, BLOCKS, block, 0)

        @pl.when(step < steps)
        def _():
            for copy in batch_copies(step + 1):
                copy.start()

        def update(unit, first, last):
            for side, sub, p, y, acc, old in ((0, 16, p_in, y_in, acc_in, old_in),
                                              (1, 64, p_out, y_out, acc_out, old_out)):
                def piece_step(s, _, side=side, sub=sub, p=p, y=y, acc=acc, old=old):
                    at = pl.ds(pl.multiple_of(unit * piece[side] + s * sub, sub), sub)

                    def mix(total, kind):
                        for where in range(4):
                            total = total + recvs[side][slot, kind, where, at].astype(F32)
                        return total / 5.0

                    g_b = acc[at].astype(BF16)
                    g = g_b.astype(F32)
                    if first:
                        tracker = g
                    else:
                        tracker = (mix(y[at], 1) + g) - old[at].astype(F32)
                    y[at] = tracker
                    if not last:
                        old[at] = g_b
                        weights = mix(p[at], 0) - LEARN_RATE * tracker
                        p[at] = weights
                        sends[side][0, at] = weights.astype(BF16)
                        sends[side][1, at] = tracker.astype(BF16)
                    return 0

                lax.fori_loop(0, piece[side] // sub, piece_step, 0)

        first_kind = jnp.where(step < steps - 1, 0, 1)

        def unit_step(unit, _):
            ahead = jnp.logical_and(step < steps, unit == UNITS - 1)

            @pl.when(ahead)
            def _():
                forward(0, first_kind, 0, 1 - slot)

            @pl.when(step < steps)
            def _():
                settle(0, unit, slot)

            @pl.when(step > 0)
            def _():
                settle(1, unit, slot)

            @pl.when(step == 0)
            def _():
                update(unit, True, False)

            @pl.when(jnp.logical_not(edge))
            def _():
                update(unit, False, False)

            @pl.when(step == steps)
            def _():
                update(unit, False, True)

            @pl.when(step < steps - 1)
            def _():
                send_piece(0, unit, 1 - slot)

            @pl.when(step < steps)
            def _():
                send_piece(1, unit, 1 - slot)

            @pl.when(jnp.logical_and(jnp.logical_not(edge), unit < UNITS // 2))
            def _():
                for side in (0, 1):
                    forward(side, 1, unit + UNITS // 2, slot)

            @pl.when(jnp.logical_and(jnp.logical_not(edge), unit < UNITS // 2 - 1))
            def _():
                for side in (0, 1):
                    forward(side, 0, unit + UNITS // 2 + 1, slot)

            @pl.when(ahead)
            def _():
                forward(1, first_kind, 0, 1 - slot)

            return 0

        lax.fori_loop(0, UNITS, unit_step, 0)
        return 0

    lax.fori_loop(0, steps + 1, phase, 0)


def solution(mesh):
    n_x, n_y = mesh.shape['tx'], mesh.shape['ty']

    def device_fn(w_in, w_out, inputs, targets):
        layers, d, ff = w_in.shape[2:]
        batches, rows = inputs.shape[2:4]
        dims = (n_x, n_y, layers, d, ff, batches - 1, rows)
        s_in, s_out = (layers * d, ff), (layers * ff, d)
        rb_rows = rows // BLOCKS
        vmem = pltpu.VMEM
        outs = pl.pallas_call(
            functools.partial(kernel, dims),
            out_shape=[vmem(s, F32) for s in (s_in, s_out, s_in, s_out)],
            in_specs=[pl.BlockSpec(memory_space=pl.ANY)] * 4,
            out_specs=[pl.BlockSpec(memory_space=vmem)] * 4,
            scratch_shapes=[
                vmem(s_in, F32), vmem(s_out, F32), vmem(s_in, BF16), vmem(s_out, BF16),
                vmem((2,) + s_in, BF16), vmem((2,) + s_out, BF16),
                vmem((2, 2, 4) + s_in, BF16), vmem((2, 2, 4) + s_out, BF16),
                vmem((rows, d), BF16), vmem((rows, d), BF16),
                vmem((layers, rb_rows, ff), F32), vmem((layers, rb_rows, ff), BF16),
                vmem((layers, rb_rows, d), BF16), vmem((rb_rows, ff), F32), vmem((rb_rows, ff), BF16),
                pltpu.SemaphoreType.DMA((2, 2, 2, UNITS, 4)),
                pltpu.SemaphoreType.DMA((2, 2, UNITS, 4)),
                pltpu.SemaphoreType.DMA((2,)),
                pltpu.SemaphoreType.DMA((2, UNITS)),
            ],
            compiler_params=pltpu.CompilerParams(
                collective_id=0, has_side_effects=True, vmem_limit_bytes=VMEM_LIMIT),
        )(w_in.reshape(s_in), w_out.reshape(s_out), inputs[0, 0], targets[0, 0])
        return tuple(o.reshape(w.shape) for o, w in zip(outs, (w_in, w_out, w_in, w_out)))

    block_spec = P('tx', 'ty')
    return jax.shard_map(device_fn, mesh=mesh, in_specs=(block_spec,) * 4, out_specs=(block_spec,) * 4, check_vma=False)
```

```python
import functools

import jax
import jax.numpy as jnp
from jax import lax
from jax.experimental import pallas as pl
from jax.experimental.pallas import tpu as pltpu
from jax.sharding import PartitionSpec as P

EPS = 1e-6
LEARN_RATE = 0.125
VMEM_LIMIT = 54 * 1024 * 1024
UNITS = 8
BLOCKS = 8
GELU_C0 = 0.7978845608028654
GELU_C1 = 0.044715 * GELU_C0
F32 = jnp.float32
BF16 = jnp.bfloat16
MESH = pl.DeviceIdType.MESH


def dot(lhs, rhs, lhs_dim, rhs_dim):
    return lax.dot_general(lhs, rhs, (((lhs_dim,), (rhs_dim,)), ((), ())), preferred_element_type=F32)


def kernel(dims, win_hbm, wout_hbm, x_hbm, tgt_hbm, p_in, p_out, y_in, y_out, acc_in, acc_out, old_in, old_out,
           send_in, send_out, recv_in, recv_out, x_v, tgt_v, gp, act, unit_in, dz,
           recv_sem, send_sem, load_sem, weight_sem):
    n_x, n_y, layers, d, ff, steps, rows = dims
    rb_rows = rows // BLOCKS
    ix, iy = lax.axis_index('tx'), lax.axis_index('ty')
    px, py = ix % 2, iy % 2
    partner = ix + 1 - 2 * px
    opposite = n_x - 1 - ix
    y_partner = iy + 1 - 2 * py
    relay_to = (iy + 2 * (1 - 2 * py) + n_y) % n_y
    relay_from = (iy - 2 * (1 - 2 * py) + n_y) % n_y
    to_partner = {'tx': partner, 'ty': iy}
    to_opposite = {'tx': opposite, 'ty': iy}
    to_y = {'tx': ix, 'ty': y_partner}
    to_z = {'tx': ix, 'ty': relay_to}
    y_dir = 3 - py
    z_dir = 2 + py

    barrier = pltpu.get_barrier_semaphore()
    for peer in (to_partner, to_opposite, to_y, to_z, {'tx': ix, 'ty': relay_from}):
        pl.semaphore_signal(barrier, inc=1, device_id=peer, device_id_type=MESH)

    piece = ((layers * d) // UNITS, (layers * ff) // UNITS)
    sends = (send_in, send_out)
    recvs = (recv_in, recv_out)

    def span(side, unit):
        return pl.ds(pl.multiple_of(unit * piece[side], piece[side]), piece[side])

    def direct(side, kind, unit, slot, dest):
        peer, where = ((to_partner, px), (to_opposite, 1 - px), (to_y, 2 + py))[dest]
        at = span(side, unit)
        return pltpu.make_async_remote_copy(
            src_ref=sends[side].at[kind, at],
            dst_ref=recvs[side].at[slot, kind, where, at],
            send_sem=send_sem.at[side, kind, unit, dest],
            recv_sem=recv_sem.at[side, slot, kind, unit, where],
            device_id=peer, device_id_type=MESH)

    def relay(side, kind, unit, slot):
        at = span(side, unit)
        return pltpu.make_async_remote_copy(
            src_ref=recvs[side].at[slot, kind, y_dir, at],
            dst_ref=recvs[side].at[slot, kind, z_dir, at],
            send_sem=send_sem.at[side, kind, unit, 3],
            recv_sem=recv_sem.at[side, slot, kind, unit, z_dir],
            device_id=to_z, device_id_type=MESH)

    def arrival(side, kind, unit, slot, where):
        at = span(side, unit)
        return pltpu.make_async_remote_copy(
            src_ref=sends[side].at[kind, at],
            dst_ref=recvs[side].at[slot, kind, where, at],
            send_sem=send_sem.at[side, kind, unit, 0],
            recv_sem=recv_sem.at[side, slot, kind, unit, where],
            device_id=to_partner, device_id_type=MESH)

    def send_piece(kind, unit, slot):
        for side in (0, 1):
            for dest in (2, 1, 0):
                direct(side, kind, unit, slot, dest).start()

    def forward(side, kind, unit, slot):
        arrival(side, kind, unit, slot, y_dir).wait_recv()
        relay(side, kind, unit, slot).start()

    def settle(kind, unit, slot):
        for side in (0, 1):
            for where in (0, 1, z_dir):
                arrival(side, kind, unit, slot, where).wait_recv()
            for dest in (0, 1, 2):
                direct(side, kind, unit, slot, dest).wait_send()
            relay(side, kind, unit, slot).wait_send()

    def batch_copies(step):
        return (pltpu.make_async_copy(x_hbm.at[step], x_v, load_sem.at[0]),
                pltpu.make_async_copy(tgt_hbm.at[step], tgt_v, load_sem.at[1]))

    def weight_copies(unit):
        return [pltpu.make_async_copy(src.at[span(side, unit)], dst.at[span(side, unit)], weight_sem.at[side, unit])
                for side, src, dst in ((0, win_hbm, p_in), (1, wout_hbm, p_out))]

    def first_load(unit, _):
        for copy in weight_copies(unit):
            copy.start()
        return 0

    lax.fori_loop(0, UNITS, first_load, 0)
    for copy in batch_copies(0):
        copy.start()

    pl.semaphore_wait(barrier, 5)

    def first_send(unit, _):
        for side, weights in ((0, p_in), (1, p_out)):
            weight_copies(unit)[side].wait()
            at = span(side, unit)
            sends[side][0, at] = weights[at].astype(BF16)
            for dest in (2, 1, 0):
                direct(side, 0, unit, 0, dest).start()
        return 0

    lax.fori_loop(0, UNITS, first_send, 0)

    def forward_layer(layer, hidden):
        w_in = send_in[0, layer * d:(layer + 1) * d]
        w_out = send_out[0, layer * ff:(layer + 1) * ff]
        inv_rms = lax.rsqrt(jnp.mean(hidden * hidden, axis=-1, keepdims=True) + EPS)
        normed = (hidden * inv_rms).astype(BF16)
        unit_in[layer] = normed
        cols = ff // 4
        for f in range(4):
            at = slice(f * cols, (f + 1) * cols)
            z = dot(normed, w_in[:, at], 1, 0)
            z2 = z * z
            tanh = jnp.tanh(z * (GELU_C0 + GELU_C1 * z2))
            cdf = 0.5 + 0.5 * tanh
            act[layer, :, at] = (z * cdf).astype(BF16)
            gp[layer, :, at] = cdf + (0.5 * z * (1.0 - tanh * tanh)) * (GELU_C0 + (3.0 * GELU_C1) * z2)
        out = dot(act[layer], w_out, 1, 0)
        return (hidden + out).astype(BF16).astype(F32), inv_rms

    def backward_layer(layer, grad_b, hidden, inv_rms):
        w_in = send_in[0, layer * d:(layer + 1) * d]
        w_out = send_out[0, layer * ff:(layer + 1) * ff]
        rows_f = ff // 4
        for f in range(4):
            at = slice(f * rows_f, (f + 1) * rows_f)
            da = dot(grad_b, w_out[at], 1, 1).astype(BF16).astype(F32)
            dz[:, at] = (da * gp[layer, :, at]).astype(BF16)
        acc_out[layer * ff:(layer + 1) * ff] += dot(act[layer], grad_b, 0, 0)
        acc_in[layer * d:(layer + 1) * d] += dot(unit_in[layer], dz[...], 0, 0)
        if layer == 0:
            return None
        du = dot(dz[...], w_in, 1, 1).astype(BF16).astype(F32)
        proj = jnp.sum(du * hidden, axis=-1, keepdims=True) * (1.0 / d)
        grad = grad_b.astype(F32) + (du * inv_rms - hidden * (proj * (inv_rms * inv_rms * inv_rms)))
        return grad.astype(BF16)

    def phase(step, _):
        slot = step % 2
        for copy in batch_copies(step):
            copy.wait()
        acc_in[...] = jnp.zeros_like(acc_in)
        acc_out[...] = jnp.zeros_like(acc_out)
        edge = jnp.logical_or(step == 0, step == steps)

        def block(rb, _):
            pair = jnp.where(step == 0, rb, jnp.where(step == steps, jnp.minimum(rb + 1, BLOCKS - 1), rb + 1))
            kind = jnp.where(step == 0, 0, jnp.where(step == steps, 1, pair % 2))
            unit = jnp.where(edge, pair, pair // 2)
            late = jnp.logical_and(step == steps, rb >= BLOCKS - 2)
            early = jnp.logical_and(step == 0, rb == BLOCKS - 1)
            last = rb == BLOCKS - 1
            at = pl.ds(pl.multiple_of(rb * rb_rows, rb_rows), rb_rows)
            hidden = [x_v[at].astype(F32)]
            scales = []
            for layer in range(layers):
                nxt, inv_rms = forward_layer(layer, hidden[-1])
                hidden.append(nxt)
                scales.append(inv_rms)

            @pl.when(jnp.logical_not(jnp.logical_and(edge, last)))
            def _():
                forward(0, kind, unit, slot)

            @pl.when(jnp.logical_and(late, last))
            def _():
                forward(1, kind, unit, slot)

            grad = ((hidden[-1] - tgt_v[at].astype(F32)) * (2.0 / (rows * d))).astype(BF16)
            for layer in reversed(range(layers)):
                grad = backward_layer(layer, grad, hidden[layer], scales[layer])

            @pl.when(jnp.logical_not(jnp.logical_or(late, early)))
            def _():
                forward(1, kind, unit, slot)

            @pl.when(early)
            def _():
                forward(0, kind, unit, slot)

            return 0

        lax.fori_loop(0, BLOCKS, block, 0)

        @pl.when(step < steps)
        def _():
            for copy in batch_copies(step + 1):
                copy.start()

        def update(unit, first, last):
            for side, sub, p, y, acc, old in ((0, 16, p_in, y_in, acc_in, old_in),
                                              (1, 64, p_out, y_out, acc_out, old_out)):
                def piece_step(s, _, side=side, sub=sub, p=p, y=y, acc=acc, old=old):
                    at = pl.ds(pl.multiple_of(unit * piece[side] + s * sub, sub), sub)

                    def mix(total, kind):
                        for where in range(4):
                            total = total + recvs[side][slot, kind, where, at].astype(F32)
                        return total / 5.0

                    g_b = acc[at].astype(BF16)
                    g = g_b.astype(F32)
                    if first:
                        tracker = g
                    else:
                        tracker = (mix(y[at], 1) + g) - old[at].astype(F32)
                    y[at] = tracker
                    if not last:
                        old[at] = g_b
                        weights = mix(p[at], 0) - LEARN_RATE * tracker
                        p[at] = weights
                        sends[side][0, at] = weights.astype(BF16)
                        sends[side][1, at] = tracker.astype(BF16)
                    return 0

                lax.fori_loop(0, piece[side] // sub, piece_step, 0)

        first_kind = jnp.where(step < steps - 1, 0, 1)

        def unit_step(unit, _):
            ahead = jnp.logical_and(step < steps, unit == UNITS - 1)

            @pl.when(ahead)
            def _():
                forward(0, first_kind, 0, 1 - slot)

            @pl.when(step < steps)
            def _():
                settle(0, unit, slot)

            @pl.when(step > 0)
            def _():
                settle(1, unit, slot)

            @pl.when(step == 0)
            def _():
                update(unit, True, False)

            @pl.when(jnp.logical_not(edge))
            def _():
                update(unit, False, False)

            @pl.when(step == steps)
            def _():
                update(unit, False, True)

            @pl.when(step < steps - 1)
            def _():
                send_piece(0, unit, 1 - slot)

            @pl.when(step < steps)
            def _():
                send_piece(1, unit, 1 - slot)

            @pl.when(jnp.logical_and(step == 0, unit == 0))
            def _():
                forward(1, 0, UNITS - 1, slot)

            @pl.when(jnp.logical_and(jnp.logical_not(edge), unit < UNITS // 2))
            def _():
                for side in (0, 1):
                    forward(side, 1, unit + UNITS // 2, slot)

            @pl.when(jnp.logical_and(jnp.logical_not(edge), unit < UNITS // 2 - 1))
            def _():
                for side in (0, 1):
                    forward(side, 0, unit + UNITS // 2 + 1, slot)

            @pl.when(ahead)
            def _():
                forward(1, first_kind, 0, 1 - slot)

            return 0

        lax.fori_loop(0, UNITS, unit_step, 0)
        return 0

    lax.fori_loop(0, steps + 1, phase, 0)


def solution(mesh):
    n_x, n_y = mesh.shape['tx'], mesh.shape['ty']

    def device_fn(w_in, w_out, inputs, targets):
        layers, d, ff = w_in.shape[2:]
        batches, rows = inputs.shape[2:4]
        dims = (n_x, n_y, layers, d, ff, batches - 1, rows)
        s_in, s_out = (layers * d, ff), (layers * ff, d)
        rb_rows = rows // BLOCKS
        vmem = pltpu.VMEM
        outs = pl.pallas_call(
            functools.partial(kernel, dims),
            out_shape=[vmem(s, F32) for s in (s_in, s_out, s_in, s_out)],
            in_specs=[pl.BlockSpec(memory_space=pl.ANY)] * 4,
            out_specs=[pl.BlockSpec(memory_space=vmem)] * 4,
            scratch_shapes=[
                vmem(s_in, F32), vmem(s_out, F32), vmem(s_in, BF16), vmem(s_out, BF16),
                vmem((2,) + s_in, BF16), vmem((2,) + s_out, BF16),
                vmem((2, 2, 4) + s_in, BF16), vmem((2, 2, 4) + s_out, BF16),
                vmem((rows, d), BF16), vmem((rows, d), BF16),
                vmem((layers, rb_rows, ff), F32), vmem((layers, rb_rows, ff), BF16),
                vmem((layers, rb_rows, d), BF16), vmem((rb_rows, ff), BF16),
                pltpu.SemaphoreType.DMA((2, 2, 2, UNITS, 4)),
                pltpu.SemaphoreType.DMA((2, 2, UNITS, 4)),
                pltpu.SemaphoreType.DMA((2,)),
                pltpu.SemaphoreType.DMA((2, UNITS)),
            ],
            compiler_params=pltpu.CompilerParams(
                collective_id=0, has_side_effects=True, vmem_limit_bytes=VMEM_LIMIT),
        )(w_in.reshape(s_in), w_out.reshape(s_out), inputs[0, 0], targets[0, 0])
        return tuple(o.reshape(w.shape) for o, w in zip(outs, (w_in, w_out, w_in, w_out)))

    block_spec = P('tx', 'ty')
    return jax.shard_map(device_fn, mesh=mesh, in_specs=(block_spec,) * 4, out_specs=(block_spec,) * 4, check_vma=False)
```

```python
import functools

import jax
import jax.numpy as jnp
from jax import lax
from jax.experimental import pallas as pl
from jax.experimental.pallas import tpu as pltpu
from jax.sharding import PartitionSpec as P

EPS = 1e-6
LEARN_RATE = 0.125
VMEM_LIMIT = 54 * 1024 * 1024
UNITS = 8
BLOCKS = 8
RELAYED = 5
GELU_C0 = 0.7978845608028654
GELU_C1 = 0.044715 * GELU_C0
F32 = jnp.float32
BF16 = jnp.bfloat16
MESH = pl.DeviceIdType.MESH


def dot(lhs, rhs, lhs_dim, rhs_dim):
    return lax.dot_general(lhs, rhs, (((lhs_dim,), (rhs_dim,)), ((), ())), preferred_element_type=F32)


def kernel(dims, win_hbm, wout_hbm, x_hbm, tgt_hbm, p_in, p_out, y_in, y_out, acc_in, acc_out, old_in, old_out,
           send_in, send_out, recv_in, recv_out, x_v, tgt_v, gp, act, unit_in, dz,
           recv_sem, send_sem, load_sem, weight_sem):
    n_x, n_y, layers, d, ff, steps, rows = dims
    rb_rows = rows // BLOCKS
    ix, iy = lax.axis_index('tx'), lax.axis_index('ty')
    px, py = ix % 2, iy % 2
    partner = ix + 1 - 2 * px
    opposite = n_x - 1 - ix
    y_partner = iy + 1 - 2 * py
    relay_to = (iy + 2 * (1 - 2 * py) + n_y) % n_y
    relay_from = (iy - 2 * (1 - 2 * py) + n_y) % n_y
    to_partner = {'tx': partner, 'ty': iy}
    to_opposite = {'tx': opposite, 'ty': iy}
    to_y = {'tx': ix, 'ty': y_partner}
    to_z = {'tx': ix, 'ty': relay_to}
    y_dir = 3 - py
    z_dir = 2 + py

    piece = ((layers * d) // UNITS, (layers * ff) // UNITS)
    sends = (send_in, send_out)
    recvs = (recv_in, recv_out)

    def span(side, unit):
        return pl.ds(pl.multiple_of(unit * piece[side], piece[side]), piece[side])

    def direct(side, kind, unit, slot, dest):
        peer, where = ((to_partner, px), (to_opposite, 1 - px), (to_y, 2 + py))[dest]
        at = span(side, unit)
        return pltpu.make_async_remote_copy(
            src_ref=sends[side].at[kind, at],
            dst_ref=recvs[side].at[slot, kind, where, at],
            send_sem=send_sem.at[side, kind, unit, dest],
            recv_sem=recv_sem.at[side, slot, kind, unit, where],
            device_id=peer, device_id_type=MESH)

    def relay(side, kind, unit, slot):
        at = span(side, unit)
        return pltpu.make_async_remote_copy(
            src_ref=recvs[side].at[slot, kind, y_dir, at],
            dst_ref=recvs[side].at[slot, kind, z_dir, at],
            send_sem=send_sem.at[side, kind, unit, 3],
            recv_sem=recv_sem.at[side, slot, kind, unit, z_dir],
            device_id=to_z, device_id_type=MESH)

    def arrival(side, kind, unit, slot, where):
        at = span(side, unit)
        return pltpu.make_async_remote_copy(
            src_ref=sends[side].at[kind, at],
            dst_ref=recvs[side].at[slot, kind, where, at],
            send_sem=send_sem.at[side, kind, unit, 0],
            recv_sem=recv_sem.at[side, slot, kind, unit, where],
            device_id=to_partner, device_id_type=MESH)

    def send_piece(kind, unit, slot):
        for side in (0, 1):
            for dest in (2, 1, 0):
                direct(side, kind, unit, slot, dest).start()

    def forward(side, kind, unit, slot):
        arrival(side, kind, unit, slot, y_dir).wait_recv()
        relay(side, kind, unit, slot).start()

    def settle(kind, unit, slot):
        for side in (0, 1):
            for where in (0, 1, z_dir):
                arrival(side, kind, unit, slot, where).wait_recv()
            for dest in (0, 1, 2):
                direct(side, kind, unit, slot, dest).wait_send()
            relay(side, kind, unit, slot).wait_send()

    def batch_copies(step):
        return (pltpu.make_async_copy(x_hbm.at[step], x_v, load_sem.at[0]),
                pltpu.make_async_copy(tgt_hbm.at[step], tgt_v, load_sem.at[1]))

    def weight_copies(unit):
        return [pltpu.make_async_copy(src.at[span(side, unit)], dst.at[span(side, unit)], weight_sem.at[side, unit])
                for side, src, dst in ((0, win_hbm, p_in), (1, wout_hbm, p_out))]

    for copy in weight_copies(0):
        copy.start()
    barrier = pltpu.get_barrier_semaphore()
    for peer in (to_partner, to_opposite, to_y, to_z, {'tx': ix, 'ty': relay_from}):
        pl.semaphore_signal(barrier, inc=1, device_id=peer, device_id_type=MESH)

    def first_piece(unit, wait):
        for side, weights in ((0, p_in), (1, p_out)):
            weight_copies(unit)[side].wait()
            at = span(side, unit)
            sends[side][0, at] = weights[at].astype(BF16)
            if wait and side == 0:
                pl.semaphore_wait(barrier, 5)
            for dest in (2, 1, 0):
                direct(side, 0, unit, 0, dest).start()

    first_piece(0, True)

    def first_load(unit, _):
        for copy in weight_copies(unit):
            copy.start()
        return 0

    lax.fori_loop(1, UNITS, first_load, 0)
    for copy in batch_copies(0):
        copy.start()

    def first_send(unit, _):
        first_piece(unit, False)
        return 0

    lax.fori_loop(1, UNITS, first_send, 0)

    def forward_layer(layer, hidden):
        w_in = send_in[0, layer * d:(layer + 1) * d]
        w_out = send_out[0, layer * ff:(layer + 1) * ff]
        inv_rms = lax.rsqrt(jnp.mean(hidden * hidden, axis=-1, keepdims=True) + EPS)
        normed = (hidden * inv_rms).astype(BF16)
        unit_in[layer] = normed
        cols = ff // 4
        for f in range(4):
            at = slice(f * cols, (f + 1) * cols)
            z = dot(normed, w_in[:, at], 1, 0)
            z2 = z * z
            tanh = jnp.tanh(z * (GELU_C0 + GELU_C1 * z2))
            cdf = 0.5 + 0.5 * tanh
            act[layer, :, at] = (z * cdf).astype(BF16)
            gp[layer, :, at] = cdf + (0.5 * z * (1.0 - tanh * tanh)) * (GELU_C0 + (3.0 * GELU_C1) * z2)
        out = dot(act[layer], w_out, 1, 0)
        return (hidden + out).astype(BF16).astype(F32), inv_rms

    def backward_layer(layer, grad_b, hidden, inv_rms):
        w_in = send_in[0, layer * d:(layer + 1) * d]
        w_out = send_out[0, layer * ff:(layer + 1) * ff]
        rows_f = ff // 4
        for f in range(4):
            at = slice(f * rows_f, (f + 1) * rows_f)
            da = dot(grad_b, w_out[at], 1, 1).astype(BF16).astype(F32)
            dz[:, at] = (da * gp[layer, :, at]).astype(BF16)
        acc_out[layer * ff:(layer + 1) * ff] += dot(act[layer], grad_b, 0, 0)
        acc_in[layer * d:(layer + 1) * d] += dot(unit_in[layer], dz[...], 0, 0)
        if layer == 0:
            return None
        du = dot(dz[...], w_in, 1, 1).astype(BF16).astype(F32)
        proj = jnp.sum(du * hidden, axis=-1, keepdims=True) * (1.0 / d)
        grad = grad_b.astype(F32) + (du * inv_rms - hidden * (proj * (inv_rms * inv_rms * inv_rms)))
        return grad.astype(BF16)

    def phase(step, _):
        slot = step % 2
        for copy in batch_copies(step):
            copy.wait()
        acc_in[...] = jnp.zeros_like(acc_in)
        acc_out[...] = jnp.zeros_like(acc_out)
        edge = jnp.logical_or(step == 0, step == steps)

        def block(rb, _):
            pair = jnp.where(step == 0, rb, jnp.where(step == steps, jnp.minimum(rb + 1, BLOCKS - 1), rb + 2))
            kind = jnp.where(step == 0, 0, jnp.where(step == steps, 1, pair % 2))
            unit = jnp.where(edge, pair, pair // 2)
            late = jnp.logical_and(step == steps, rb >= BLOCKS - 2)
            early = jnp.logical_and(step == 0, rb == BLOCKS - 1)
            last = rb == BLOCKS - 1
            at = pl.ds(pl.multiple_of(rb * rb_rows, rb_rows), rb_rows)
            hidden = [x_v[at].astype(F32)]
            scales = []
            for layer in range(layers):
                nxt, inv_rms = forward_layer(layer, hidden[-1])
                hidden.append(nxt)
                scales.append(inv_rms)

            @pl.when(jnp.logical_not(jnp.logical_and(edge, last)))
            def _():
                forward(0, kind, unit, slot)

            @pl.when(jnp.logical_and(late, last))
            def _():
                forward(1, kind, unit, slot)

            grad = ((hidden[-1] - tgt_v[at].astype(F32)) * (2.0 / (rows * d))).astype(BF16)
            for layer in reversed(range(layers)):
                grad = backward_layer(layer, grad, hidden[layer], scales[layer])

            @pl.when(jnp.logical_not(jnp.logical_or(late, early)))
            def _():
                forward(1, kind, unit, slot)

            @pl.when(early)
            def _():
                forward(0, kind, unit, slot)

            return 0

        lax.fori_loop(0, BLOCKS, block, 0)

        @pl.when(step < steps)
        def _():
            for copy in batch_copies(step + 1):
                copy.start()

        def update(unit, first, last):
            for side, sub, p, y, acc, old in ((0, 16, p_in, y_in, acc_in, old_in),
                                              (1, 64, p_out, y_out, acc_out, old_out)):
                def piece_step(s, _, side=side, sub=sub, p=p, y=y, acc=acc, old=old):
                    at = pl.ds(pl.multiple_of(unit * piece[side] + s * sub, sub), sub)

                    def mix(total, kind):
                        for where in range(4):
                            total = total + recvs[side][slot, kind, where, at].astype(F32)
                        return total / 5.0

                    g_b = acc[at].astype(BF16)
                    g = g_b.astype(F32)
                    if first:
                        tracker = g
                    else:
                        tracker = (mix(y[at], 1) + g) - old[at].astype(F32)
                    y[at] = tracker
                    if not last:
                        old[at] = g_b
                        weights = mix(p[at], 0) - LEARN_RATE * tracker
                        p[at] = weights
                        sends[side][0, at] = weights.astype(BF16)
                        sends[side][1, at] = tracker.astype(BF16)
                    return 0

                lax.fori_loop(0, piece[side] // sub, piece_step, 0)

        first_kind = jnp.where(step < steps - 1, 0, 1)

        def unit_step(unit, _):
            ahead = jnp.logical_and(step < steps, unit == UNITS - 1)

            @pl.when(ahead)
            def _():
                for side in (0, 1):
                    forward(side, first_kind, 0, 1 - slot)

            @pl.when(jnp.logical_and(ahead, step < steps - 1))
            def _():
                for side in (0, 1):
                    forward(side, 1, 0, 1 - slot)

            @pl.when(step < steps)
            def _():
                settle(0, unit, slot)

            @pl.when(step > 0)
            def _():
                settle(1, unit, slot)

            @pl.when(step == 0)
            def _():
                update(unit, True, False)

            @pl.when(jnp.logical_not(edge))
            def _():
                update(unit, False, False)

            @pl.when(step == steps)
            def _():
                update(unit, False, True)

            @pl.when(step < steps - 1)
            def _():
                send_piece(0, unit, 1 - slot)

            @pl.when(step < steps)
            def _():
                send_piece(1, unit, 1 - slot)

            @pl.when(jnp.logical_and(step == 0, unit == 0))
            def _():
                forward(1, 0, UNITS - 1, slot)

            @pl.when(jnp.logical_and(jnp.logical_not(edge), unit < UNITS - RELAYED))
            def _():
                for kind in (0, 1):
                    for side in (0, 1):
                        forward(side, kind, unit + RELAYED, slot)

            return 0

        lax.fori_loop(0, UNITS, unit_step, 0)
        return 0

    lax.fori_loop(0, steps + 1, phase, 0)


def solution(mesh):
    n_x, n_y = mesh.shape['tx'], mesh.shape['ty']

    def device_fn(w_in, w_out, inputs, targets):
        layers, d, ff = w_in.shape[2:]
        batches, rows = inputs.shape[2:4]
        dims = (n_x, n_y, layers, d, ff, batches - 1, rows)
        s_in, s_out = (layers * d, ff), (layers * ff, d)
        rb_rows = rows // BLOCKS
        vmem = pltpu.VMEM
        outs = pl.pallas_call(
            functools.partial(kernel, dims),
            out_shape=[vmem(s, F32) for s in (s_in, s_out, s_in, s_out)],
            in_specs=[pl.BlockSpec(memory_space=pl.ANY)] * 4,
            out_specs=[pl.BlockSpec(memory_space=vmem)] * 4,
            scratch_shapes=[
                vmem(s_in, F32), vmem(s_out, F32), vmem(s_in, BF16), vmem(s_out, BF16),
                vmem((2,) + s_in, BF16), vmem((2,) + s_out, BF16),
                vmem((2, 2, 4) + s_in, BF16), vmem((2, 2, 4) + s_out, BF16),
                vmem((rows, d), BF16), vmem((rows, d), BF16),
                vmem((layers, rb_rows, ff), F32), vmem((layers, rb_rows, ff), BF16),
                vmem((layers, rb_rows, d), BF16), vmem((rb_rows, ff), BF16),
                pltpu.SemaphoreType.DMA((2, 2, 2, UNITS, 4)),
                pltpu.SemaphoreType.DMA((2, 2, UNITS, 4)),
                pltpu.SemaphoreType.DMA((2,)),
                pltpu.SemaphoreType.DMA((2, UNITS)),
            ],
            compiler_params=pltpu.CompilerParams(
                collective_id=0, has_side_effects=True, vmem_limit_bytes=VMEM_LIMIT),
        )(w_in.reshape(s_in), w_out.reshape(s_out), inputs[0, 0], targets[0, 0])
        return tuple(o.reshape(w.shape) for o, w in zip(outs, (w_in, w_out, w_in, w_out)))

    block_spec = P('tx', 'ty')
    return jax.shard_map(device_fn, mesh=mesh, in_specs=(block_spec,) * 4, out_specs=(block_spec,) * 4, check_vma=False)
```

```python
import functools

import jax
import jax.numpy as jnp
from jax import lax
from jax.experimental import pallas as pl
from jax.experimental.pallas import tpu as pltpu
from jax.sharding import PartitionSpec as P

EPS = 1e-6
LEARN_RATE = 0.125
VMEM_LIMIT = 54 * 1024 * 1024
UNITS = 8
BLOCKS = 8
RELAYED = 5
GELU_C0 = 0.7978845608028654
GELU_C1 = 0.044715 * GELU_C0
F32 = jnp.float32
BF16 = jnp.bfloat16
MESH = pl.DeviceIdType.MESH


def dot(lhs, rhs, lhs_dim, rhs_dim):
    return lax.dot_general(lhs, rhs, (((lhs_dim,), (rhs_dim,)), ((), ())), preferred_element_type=F32)


def kernel(dims, win_hbm, wout_hbm, x_hbm, tgt_hbm, p_in, p_out, y_in, y_out, acc_in, acc_out, old_in, old_out,
           send_in, send_out, recv_in, recv_out, x_v, tgt_v, gp, act, unit_in, dz,
           recv_sem, send_sem, load_sem, weight_sem):
    n_x, n_y, layers, d, ff, steps, rows = dims
    rb_rows = rows // BLOCKS
    ix, iy = lax.axis_index('tx'), lax.axis_index('ty')
    px, py = ix % 2, iy % 2
    partner = ix + 1 - 2 * px
    opposite = n_x - 1 - ix
    y_partner = iy + 1 - 2 * py
    relay_to = (iy + 2 * (1 - 2 * py) + n_y) % n_y
    relay_from = (iy - 2 * (1 - 2 * py) + n_y) % n_y
    to_partner = {'tx': partner, 'ty': iy}
    to_opposite = {'tx': opposite, 'ty': iy}
    to_y = {'tx': ix, 'ty': y_partner}
    to_z = {'tx': ix, 'ty': relay_to}
    y_dir = 3 - py
    z_dir = 2 + py

    piece = ((layers * d) // UNITS, (layers * ff) // UNITS)
    sends = (send_in, send_out)
    recvs = (recv_in, recv_out)

    def span(side, unit):
        return pl.ds(pl.multiple_of(unit * piece[side], piece[side]), piece[side])

    def direct(side, kind, unit, slot, dest):
        peer, where = ((to_partner, px), (to_opposite, 1 - px), (to_y, 2 + py))[dest]
        at = span(side, unit)
        return pltpu.make_async_remote_copy(
            src_ref=sends[side].at[kind, at],
            dst_ref=recvs[side].at[slot, kind, where, at],
            send_sem=send_sem.at[side, kind, unit, dest],
            recv_sem=recv_sem.at[side, slot, kind, unit, where],
            device_id=peer, device_id_type=MESH)

    def relay(side, kind, unit, slot):
        at = span(side, unit)
        return pltpu.make_async_remote_copy(
            src_ref=recvs[side].at[slot, kind, y_dir, at],
            dst_ref=recvs[side].at[slot, kind, z_dir, at],
            send_sem=send_sem.at[side, kind, unit, 3],
            recv_sem=recv_sem.at[side, slot, kind, unit, z_dir],
            device_id=to_z, device_id_type=MESH)

    def arrival(side, kind, unit, slot, where):
        at = span(side, unit)
        return pltpu.make_async_remote_copy(
            src_ref=sends[side].at[kind, at],
            dst_ref=recvs[side].at[slot, kind, where, at],
            send_sem=send_sem.at[side, kind, unit, 0],
            recv_sem=recv_sem.at[side, slot, kind, unit, where],
            device_id=to_partner, device_id_type=MESH)

    def send_piece(kind, unit, slot):
        for side in (0, 1):
            for dest in (2, 1, 0):
                direct(side, kind, unit, slot, dest).start()

    def forward(side, kind, unit, slot):
        arrival(side, kind, unit, slot, y_dir).wait_recv()
        relay(side, kind, unit, slot).start()

    def settle(kind, unit, slot):
        for side in (0, 1):
            for where in (0, 1, z_dir):
                arrival(side, kind, unit, slot, where).wait_recv()
            for dest in (0, 1, 2):
                direct(side, kind, unit, slot, dest).wait_send()
            relay(side, kind, unit, slot).wait_send()

    def batch_copies(step):
        return (pltpu.make_async_copy(x_hbm.at[step], x_v, load_sem.at[0]),
                pltpu.make_async_copy(tgt_hbm.at[step], tgt_v, load_sem.at[1]))

    def weight_copies(unit):
        return [pltpu.make_async_copy(src.at[span(side, unit)], dst.at[span(side, unit)], weight_sem.at[side, unit])
                for side, src, dst in ((0, win_hbm, p_in), (1, wout_hbm, p_out))]

    for copy in weight_copies(0):
        copy.start()
    barrier = pltpu.get_barrier_semaphore()
    for peer in (to_partner, to_opposite, to_y, to_z, {'tx': ix, 'ty': relay_from}):
        pl.semaphore_signal(barrier, inc=1, device_id=peer, device_id_type=MESH)

    def first_piece(unit, wait):
        for side, weights in ((0, p_in), (1, p_out)):
            weight_copies(unit)[side].wait()
            at = span(side, unit)
            sends[side][0, at] = weights[at].astype(BF16)
            if wait and side == 0:
                pl.semaphore_wait(barrier, 5)
            for dest in (2, 1, 0):
                direct(side, 0, unit, 0, dest).start()

    first_piece(0, True)

    def first_load(unit, _):
        for copy in weight_copies(unit):
            copy.start()
        return 0

    lax.fori_loop(1, UNITS, first_load, 0)
    for copy in batch_copies(0):
        copy.start()

    def first_send(unit, _):
        first_piece(unit, False)
        return 0

    lax.fori_loop(1, UNITS, first_send, 0)

    def forward_layer(layer, hidden):
        w_in = send_in[0, layer * d:(layer + 1) * d]
        w_out = send_out[0, layer * ff:(layer + 1) * ff]
        inv_rms = lax.rsqrt(jnp.mean(hidden * hidden, axis=-1, keepdims=True) + EPS)
        normed = (hidden * inv_rms).astype(BF16)
        unit_in[layer] = normed
        cols = ff // 4
        for f in range(4):
            at = slice(f * cols, (f + 1) * cols)
            z = dot(normed, w_in[:, at], 1, 0)
            z2 = z * z
            tanh = jnp.tanh(z * (GELU_C0 + GELU_C1 * z2))
            cdf = 0.5 + 0.5 * tanh
            act[layer, :, at] = (z * cdf).astype(BF16)
            gp[layer, :, at] = cdf + (0.5 * z * (1.0 - tanh * tanh)) * (GELU_C0 + (3.0 * GELU_C1) * z2)
        out = dot(act[layer], w_out, 1, 0)
        return (hidden + out).astype(BF16).astype(F32), inv_rms

    def backward_layer(layer, grad_b, hidden, inv_rms):
        w_in = send_in[0, layer * d:(layer + 1) * d]
        w_out = send_out[0, layer * ff:(layer + 1) * ff]
        rows_f = ff // 4
        for f in range(4):
            at = slice(f * rows_f, (f + 1) * rows_f)
            da = dot(grad_b, w_out[at], 1, 1).astype(BF16).astype(F32)
            dz[:, at] = (da * gp[layer, :, at]).astype(BF16)
        acc_out[layer * ff:(layer + 1) * ff] += dot(act[layer], grad_b, 0, 0)
        acc_in[layer * d:(layer + 1) * d] += dot(unit_in[layer], dz[...], 0, 0)
        if layer == 0:
            return None
        du = dot(dz[...], w_in, 1, 1).astype(BF16).astype(F32)
        proj = jnp.sum(du * hidden, axis=-1, keepdims=True) * (1.0 / d)
        grad = grad_b.astype(F32) + (du * inv_rms - hidden * (proj * (inv_rms * inv_rms * inv_rms)))
        return grad.astype(BF16)

    def phase(step, _):
        slot = step % 2
        for copy in batch_copies(step):
            copy.wait()
        acc_in[...] = jnp.zeros_like(acc_in)
        acc_out[...] = jnp.zeros_like(acc_out)
        edge = jnp.logical_or(step == 0, step == steps)

        def block(rb, _):
            pair = jnp.where(step == 0, rb, jnp.where(step == steps, jnp.minimum(rb + 1, BLOCKS - 1), rb + 2))
            kind = jnp.where(step == 0, 0, jnp.where(step == steps, 1, pair % 2))
            unit = jnp.where(edge, pair, pair // 2)
            late = jnp.logical_and(step == steps, rb >= BLOCKS - 2)
            early = jnp.logical_and(step == 0, rb == BLOCKS - 1)
            last = rb == BLOCKS - 1
            at = pl.ds(pl.multiple_of(rb * rb_rows, rb_rows), rb_rows)
            hidden = [x_v[at].astype(F32)]
            scales = []
            for layer in range(layers):
                nxt, inv_rms = forward_layer(layer, hidden[-1])
                hidden.append(nxt)
                scales.append(inv_rms)

            @pl.when(jnp.logical_not(jnp.logical_and(edge, last)))
            def _():
                forward(0, kind, unit, slot)

            @pl.when(jnp.logical_and(late, last))
            def _():
                forward(1, kind, unit, slot)

            grad = ((hidden[-1] - tgt_v[at].astype(F32)) * (2.0 / (rows * d))).astype(BF16)
            for layer in reversed(range(layers)):
                grad = backward_layer(layer, grad, hidden[layer], scales[layer])

            @pl.when(jnp.logical_not(jnp.logical_or(late, early)))
            def _():
                forward(1, kind, unit, slot)

            @pl.when(early)
            def _():
                forward(0, kind, unit, slot)

            return 0

        lax.fori_loop(0, BLOCKS, block, 0)

        @pl.when(step < steps)
        def _():
            for copy in batch_copies(step + 1):
                copy.start()

        def update(unit, first, last):
            for side, sub, p, y, acc, old in ((0, 16, p_in, y_in, acc_in, old_in),
                                              (1, 64, p_out, y_out, acc_out, old_out)):
                def piece_step(s, _, side=side, sub=sub, p=p, y=y, acc=acc, old=old):
                    at = pl.ds(pl.multiple_of(unit * piece[side] + s * sub, sub), sub)

                    def mix(total, kind):
                        for where in range(4):
                            total = total + recvs[side][slot, kind, where, at].astype(F32)
                        return total / 5.0

                    g_b = acc[at].astype(BF16)
                    g = g_b.astype(F32)
                    if first:
                        tracker = g
                    else:
                        tracker = (mix(y[at], 1) + g) - old[at].astype(F32)
                    y[at] = tracker
                    if not last:
                        old[at] = g_b
                        weights = mix(p[at], 0) - LEARN_RATE * tracker
                        p[at] = weights
                        sends[side][0, at] = weights.astype(BF16)
                        sends[side][1, at] = tracker.astype(BF16)
                    return 0

                lax.fori_loop(0, piece[side] // sub, piece_step, 0)

        first_kind = jnp.where(step < steps - 1, 0, 1)

        def unit_step(unit, _):
            ahead = jnp.logical_and(step < steps, unit == UNITS - 1)

            @pl.when(ahead)
            def _():
                for side in (0, 1):
                    forward(side, first_kind, 0, 1 - slot)

            @pl.when(jnp.logical_and(ahead, step < steps - 1))
            def _():
                for side in (0, 1):
                    forward(side, 1, 0, 1 - slot)

            @pl.when(step < steps)
            def _():
                settle(0, unit, slot)

            @pl.when(step > 0)
            def _():
                settle(1, unit, slot)

            @pl.when(step == 0)
            def _():
                update(unit, True, False)

            @pl.when(jnp.logical_not(edge))
            def _():
                update(unit, False, False)

            @pl.when(step == steps)
            def _():
                update(unit, False, True)

            @pl.when(step < steps - 1)
            def _():
                send_piece(0, unit, 1 - slot)

            @pl.when(step < steps)
            def _():
                send_piece(1, unit, 1 - slot)

            @pl.when(jnp.logical_and(step == 0, unit == 0))
            def _():
                forward(1, 0, UNITS - 1, slot)

            @pl.when(jnp.logical_and(jnp.logical_not(edge), unit < UNITS - RELAYED))
            def _():
                for kind in (0, 1):
                    for side in (0, 1):
                        forward(side, kind, unit + RELAYED, slot)

            return 0

        lax.fori_loop(0, UNITS, unit_step, 0)
        return 0

    lax.fori_loop(0, steps + 1, phase, 0)


def store_kernel(*refs):
    count = len(refs) // 2
    copies = []
    for k in range(count):
        half = refs[k].shape[0] // 2
        for part in range(2):
            at = pl.ds(part * half, half)
            copies.append(pltpu.make_async_copy(refs[k].at[at], refs[count + k].at[at], refs[-1].at[k, part]))
    for copy in copies:
        copy.start()
    for copy in copies:
        copy.wait()


def solution(mesh):
    n_x, n_y = mesh.shape['tx'], mesh.shape['ty']

    def device_fn(w_in, w_out, inputs, targets):
        layers, d, ff = w_in.shape[2:]
        batches, rows = inputs.shape[2:4]
        dims = (n_x, n_y, layers, d, ff, batches - 1, rows)
        s_in, s_out = (layers * d, ff), (layers * ff, d)
        rb_rows = rows // BLOCKS
        vmem = pltpu.VMEM
        outs = pl.pallas_call(
            functools.partial(kernel, dims),
            out_shape=[vmem(s, F32) for s in (s_in, s_out, s_in, s_out)],
            in_specs=[pl.BlockSpec(memory_space=pl.ANY)] * 4,
            out_specs=[pl.BlockSpec(memory_space=vmem)] * 4,
            scratch_shapes=[
                vmem(s_in, F32), vmem(s_out, F32), vmem(s_in, BF16), vmem(s_out, BF16),
                vmem((2,) + s_in, BF16), vmem((2,) + s_out, BF16),
                vmem((2, 2, 4) + s_in, BF16), vmem((2, 2, 4) + s_out, BF16),
                vmem((rows, d), BF16), vmem((rows, d), BF16),
                vmem((layers, rb_rows, ff), F32), vmem((layers, rb_rows, ff), BF16),
                vmem((layers, rb_rows, d), BF16), vmem((rb_rows, ff), BF16),
                pltpu.SemaphoreType.DMA((2, 2, 2, UNITS, 4)),
                pltpu.SemaphoreType.DMA((2, 2, UNITS, 4)),
                pltpu.SemaphoreType.DMA((2,)),
                pltpu.SemaphoreType.DMA((2, UNITS)),
            ],
            compiler_params=pltpu.CompilerParams(
                collective_id=0, has_side_effects=True, vmem_limit_bytes=VMEM_LIMIT),
        )(w_in.reshape(s_in), w_out.reshape(s_out), inputs[0, 0], targets[0, 0])
        outs = pl.pallas_call(
            store_kernel,
            out_shape=[jax.ShapeDtypeStruct(s, F32) for s in (s_in, s_out, s_in, s_out)],
            in_specs=[pl.BlockSpec(memory_space=pl.ANY)] * 4,
            out_specs=[pl.BlockSpec(memory_space=pl.ANY)] * 4,
            scratch_shapes=[pltpu.SemaphoreType.DMA((4, 2))],
            compiler_params=pltpu.CompilerParams(vmem_limit_bytes=2 * 1024 * 1024),
        )(*outs)
        return tuple(o.reshape(w.shape) for o, w in zip(outs, (w_in, w_out, w_in, w_out)))

    block_spec = P('tx', 'ty')
    return jax.shard_map(device_fn, mesh=mesh, in_specs=(block_spec,) * 4, out_specs=(block_spec,) * 4, check_vma=False)
```
